32 devices in a mesh: tm: 8 (over y, x, core), space: 4 (over z).
Axes of the slice: x: 2, y: 2, z: 4, core: 2. Of those that a mesh axis runs over, the one named last changes fastest.
Arguments:
- gauge_links: float32 [8, 2, 3, 3, 3, 8, 1024], P('tm', None, None, None, None, 'space'), may hold values from -1 to 1, as said below
- time_links: float32 [8, 2, 3, 3, 8, 1024], P('tm', None, None, None, 'space'), may hold values from -1 to 1, as said below
- sink_vectors: bfloat16 [8, 2, 128, 3, 8, 1024], P('tm', None, None, None, 'space'), may hold values from -0.29882812 to 0.29882812
- source_times: int32 [4], replicated, may hold values from 0 to 7
- source_index: int32 [4, 2], replicated, may hold values from 0 to 127
- kinetic_coef: float32 [4, 2], replicated, may hold values from 0.005 to 0.12
Outputs:
- perambulator: float32 [2, 4, 2, 8, 128], P(None, None, None, 'tm', 'space')
The draws below stay inside these ranges and needn't reach their ends.
Inputs may be any that keep to these rules, and one draw needn't show every extreme that they name: `gauge_links`: each link is a special unitary 3 x 3 matrix. `time_links`: each link is a special unitary 3 x 3 matrix.
All inputs are finite; a program needn't handle non-finite values.
Results may differ from the reference program's by a relative error of at most 0.0029.
Values may be sent and summed in bfloat16 or wider, within the bound.
A program may use at most 128 MiB of HBM per device.

```python
import math
from functools import partial
import jax
import jax.numpy as jnp
from jax import lax

LS = 32
NEV = 128
SRC = 2
NSRCT = 4
NT = 8
LX = 8


def special_unitary(key, lead):
    keys = jax.random.split(key, 4)
    first = jax.random.normal(keys[0], lead + (3,), jnp.float32) + 1j * jax.random.normal(keys[1], lead + (3,), jnp.float32)
    second = jax.random.normal(keys[2], lead + (3,), jnp.float32) + 1j * jax.random.normal(keys[3], lead + (3,), jnp.float32)
    first = first / jnp.sqrt(jnp.sum(jnp.real(first) * jnp.real(first) + jnp.imag(first) * jnp.imag(first), axis=-1, keepdims=True))
    second = second - jnp.sum(jnp.conj(first) * second, axis=-1, keepdims=True) * first
    second = second / jnp.sqrt(jnp.sum(jnp.real(second) * jnp.real(second) + jnp.imag(second) * jnp.imag(second), axis=-1, keepdims=True))
    third = jnp.conj(jnp.cross(first, second))
    matrix = jnp.stack([first, second, third], axis=-2)
    return jnp.stack([jnp.real(matrix), jnp.imag(matrix)], axis=0).astype(jnp.float32)


def draw_gauge_links(key, part):
    matrices = special_unitary(jax.random.fold_in(key, 11), (NT, 3, LX, LS * LS))
    return matrices.transpose(1, 0, 2, 5, 6, 3, 4)


def draw_time_links(key, part):
    matrices = special_unitary(jax.random.fold_in(key, 23), (NT, LX, LS * LS))
    return matrices.transpose(1, 0, 4, 5, 2, 3)


def with_ends(result, own_key, smallest, top_value):
    place = [jax.random.randint(jax.random.fold_in(own_key, axis), (), 0, length) for axis, length in enumerate(result.shape)]
    widest = result.shape.index(max(result.shape))
    neighbour = place[:widest] + [(place[widest] + 1) % result.shape[widest]] + place[widest + 1:]
    return result.at[tuple(place)].set(smallest).at[tuple(neighbour)].set(top_value)


def levels(key, shape, pieces, least, top_value):
    gain, own = 1.0, jax.random.fold_in(key, 6)
    for dim, shards_of in pieces:
        steps = jnp.exp(jax.random.uniform(jax.random.fold_in(own, dim), (shards_of,), jnp.float32, least / len(pieces), top_value / len(pieces)))
        gain = gain * jnp.repeat(steps, shape[dim] // shards_of).reshape([-1 if axis == dim else 1 for axis in range(len(shape))])
    return gain


def scatter_about(stream_key, dims, deviation, most, shards=(), dtype=jnp.bfloat16):
    values = jax.random.normal(stream_key, dims, jnp.float32) * deviation
    if len(shards) > 0:
        values = levels(stream_key, dims, shards, -0.22, 0.18) * values
    return jnp.clip(values, min=-most, max=most).astype(dtype)


def setup_inputs(seed: int = 0) -> dict:
    streams_of = jax.random.split(jax.random.key(seed), 7)
    gauge_links = draw_gauge_links(jax.random.fold_in(streams_of[6], 71), 0)
    time_links = draw_time_links(jax.random.fold_in(streams_of[6], 71), 0)
    sink_vectors = scatter_about(streams_of[2], (NT, 2, NEV, 3, LX, LS * LS), 0.05, 0.29882812, ((0, 8), (4, 4)))
    source_times = with_ends(jax.random.randint(streams_of[3], (NSRCT,), 0, NT), jax.random.fold_in(streams_of[3], 1), 0, NT - 1).astype(jnp.int32)
    source_index = with_ends(jax.random.randint(streams_of[4], (NSRCT, SRC), 0, NEV), jax.random.fold_in(streams_of[4], 1), 0, NEV - 1).astype(jnp.int32)
    kinetic_coef = jnp.clip(jnp.exp(jax.random.uniform(streams_of[5], (NSRCT, SRC), jnp.float32, math.log(0.005), math.log(0.12))), 0.005, 0.12)
    return dict(gauge_links=gauge_links, time_links=time_links, sink_vectors=sink_vectors, source_times=source_times, source_index=source_index, kinetic_coef=kinetic_coef)


einsum_high = partial(jnp.einsum, precision=lax.Precision.HIGHEST)


def colour_apply(matrix, vector_in):
    real_part = einsum_high('abxs,bvxs->avxs', matrix[0], vector_in[0]) - einsum_high('abxs,bvxs->avxs', matrix[1], vector_in[1])
    imag_part = einsum_high('abxs,bvxs->avxs', matrix[0], vector_in[1]) + einsum_high('abxs,bvxs->avxs', matrix[1], vector_in[0])
    return jnp.stack([real_part, imag_part])


def colour_adjoint(matrix, vector_in):
    real_part = einsum_high('baxs,bvxs->avxs', matrix[0], vector_in[0]) + einsum_high('baxs,bvxs->avxs', matrix[1], vector_in[1])
    imag_part = einsum_high('baxs,bvxs->avxs', matrix[0], vector_in[1]) - einsum_high('baxs,bvxs->avxs', matrix[1], vector_in[0])
    return jnp.stack([real_part, imag_part])


def shift_up(values, direction):
    if direction == 0:
        return jnp.roll(values, -1, axis=3)
    if direction == 1:
        return jnp.roll(values, -LS, axis=-1)
    z_index = jnp.arange(values.shape[-1]) % LS
    return jnp.where(z_index == LS - 1, jnp.roll(values, LS - 1, axis=-1), jnp.roll(values, -1, axis=-1))


def shift_down(values, direction):
    if direction == 0:
        return jnp.roll(values, 1, axis=3)
    if direction == 1:
        return jnp.roll(values, LS, axis=-1)
    z_index = jnp.arange(values.shape[-1]) % LS
    return jnp.where(z_index == 0, jnp.roll(values, -(LS - 1), axis=-1), jnp.roll(values, 1, axis=-1))


def laplace_full(wavefn, slice_links):
    summed = -6.0 * wavefn
    for direction in range(3):
        matrix = slice_links[:, direction]
        summed = summed + colour_apply(matrix, shift_up(wavefn, direction))
        summed = summed + colour_adjoint(shift_down(matrix, direction), shift_down(wavefn, direction))
    return summed


def project_slice(sink_slice, evolved):
    rounded = evolved.astype(jnp.bfloat16).astype(jnp.float32)
    sinks = sink_slice.astype(jnp.float32)
    real_part = jnp.einsum('ecxs,cvxs->ve', sinks[0], rounded[0]) + jnp.einsum('ecxs,cvxs->ve', sinks[1], rounded[1])
    imag_part = jnp.einsum('ecxs,cvxs->ve', sinks[0], rounded[1]) - jnp.einsum('ecxs,cvxs->ve', sinks[1], rounded[0])
    return jnp.stack([real_part, imag_part])


def reference(gauge_links, time_links, sink_vectors, source_times, source_index, kinetic_coef):
    per_time = []
    for which in range(NSRCT):
        start = source_times[which].astype(jnp.int32)
        start_sinks = lax.dynamic_index_in_dim(sink_vectors, start, 0, keepdims=False)
        source = jnp.take(start_sinks, source_index[which], axis=1).astype(jnp.float32).transpose(0, 2, 1, 3, 4)
        weight = (0.5 * kinetic_coef[which]).astype(jnp.float32)[None, None, :, None, None]

        def advance_slice(rounds, state_pair):
            wavefn, correlation_table = state_pair
            slice_no = ((start + rounds) % NT).astype(jnp.int32)
            slice_links = lax.dynamic_index_in_dim(gauge_links, slice_no, 0, keepdims=False)
            time_link = lax.dynamic_index_in_dim(time_links, slice_no, 0, keepdims=False)
            sink_slice = lax.dynamic_index_in_dim(sink_vectors, slice_no, 0, keepdims=False)
            halfway = wavefn + weight * laplace_full(wavefn, slice_links)
            turned = colour_adjoint(time_link, halfway)
            evolved = turned + weight * laplace_full(turned, slice_links)
            correlations = project_slice(sink_slice, evolved)
            zero = jnp.zeros((), jnp.int32)
            correlation_table = lax.dynamic_update_slice(correlation_table, correlations[:, :, None, :], (zero, zero, slice_no, zero))
            return evolved, correlation_table

        empty = jnp.zeros((2, SRC, NT, NEV), jnp.float32)
        _, correlation_table = lax.fori_loop(0, NT, advance_slice, (source, empty))
        per_time.append(correlation_table)
    return jnp.stack(per_time, axis=1)
```

```python
import math

import jax
import jax.numpy as jnp
from jax import lax
from jax.experimental import pallas as pl
from jax.experimental.pallas import tpu as pltpu
from jax.sharding import PartitionSpec as P

LANES = 128


def roll(x, by, axis):
    size = x.shape[axis]
    return pltpu.roll(x, by % size, axis)


def apply_link(link, vec):
    real, imag = [], []
    for a in range(3):
        re = im = None
        for b in range(3):
            ur, ui = link(0, a, b), link(1, a, b)
            r = ur * vec[0][b] - ui * vec[1][b]
            i = ur * vec[1][b] + ui * vec[0][b]
            re = r if re is None else re + r
            im = i if im is None else im + i
        real.append(re)
        imag.append(im)
    return [real, imag]


def apply_both(link, vec_up, vec_here):
    up = [[None] * 3, [None] * 3]
    down = [[None] * 3, [None] * 3]

    def add(out, part, at, value):
        out[part][at] = value if out[part][at] is None else out[part][at] + value

    for a in range(3):
        for b in range(3):
            ur, ui = link(0, a, b), link(1, a, b)
            add(up, 0, a, ur * vec_up[0][b] - ui * vec_up[1][b])
            add(up, 1, a, ur * vec_up[1][b] + ui * vec_up[0][b])
            add(down, 0, b, ur * vec_here[0][a] + ui * vec_here[1][a])
            add(down, 1, b, ur * vec_here[1][a] - ui * vec_here[0][a])
    return up, down


def evolve_kernel(planes, rows, blocks, side, start_ref, place_ref, weight_ref, gauge_ref, time_ref,
                  source_ref, out_ref, field, turned):
    which, rounds = pl.program_id(0), pl.program_id(1)
    extent = planes * blocks
    weight = weight_ref[which]
    lane = lax.broadcasted_iota(jnp.int32, (planes, rows, LANES), 2)
    per_row = LANES // side

    def y_up(x):
        turned_lanes = roll(x, -side, 2)
        return jnp.where(lane < LANES - side, turned_lanes, roll(turned_lanes, -1, 1))

    def y_down(x):
        turned_lanes = roll(x, side, 2)
        return jnp.where(lane >= side, turned_lanes, roll(turned_lanes, 1, 1))

    def z_up(x):
        return jnp.where(lane % side == side - 1, roll(x, side - 1, 2), roll(x, -1, 2))

    def z_down(x):
        return jnp.where(lane % side == 0, roll(x, 1 - side, 2), roll(x, 1, 2))

    def gauge(block, direction):
        def link(part, row, column):
            at = ((part * 3 + direction) * 3 + row) * 3 + column
            value = gauge_ref[0, block, at].astype(jnp.float32)
            return value.reshape(planes, rows, LANES)
        return link

    def read(ref, first):
        return [[ref[part * 3 + c, pl.ds(first, planes)] for c in range(3)] for part in range(2)]

    def each(fn, vec):
        return [[fn(vec[part][c]) for c in range(3)] for part in range(2)]

    def plus(*vecs):
        return [[sum(v[part][c] for v in vecs[1:]) + vecs[0][part][c] for c in range(3)] for part in range(2)]

    def close(ref):
        for at in range(6):
            ref[at, pl.ds(extent, 1)] = ref[at, pl.ds(0, 1)]

    def hop(src, dst, then):
        last = read(src, extent - planes)
        _, wrapped = apply_both(gauge(blocks - 1, 0), last, last)
        carried = tuple(wrapped[part][c][planes - 1:] for part in range(2) for c in range(3))

        def one_block(block, carry):
            first = block * planes
            here = read(src, first)
            up, down = apply_both(gauge(block, 0), read(src, first + 1), here)
            flat = [down[part][c] for part in range(2) for c in range(3)]
            moved = [jnp.concatenate([low, x[: planes - 1]], axis=0) for low, x in zip(carry, flat)]
            total = plus(up, [moved[:3], moved[3:]])
            up, down = apply_both(gauge(block, 1), each(y_up, here), here)
            total = plus(total, up, each(y_down, down))
            up, down = apply_both(gauge(block, 2), each(z_up, here), here)
            total = plus(total, up, each(z_down, down))
            result = [[here[part][c] + weight * (total[part][c] - 6.0 * here[part][c]) for c in range(3)]
                      for part in range(2)]
            result = then(block, result)
            for part in range(2):
                for c in range(3):
                    dst[part * 3 + c, pl.ds(first, planes)] = result[part][c]
            return tuple(x[planes - 1:] for x in flat)

        lax.fori_loop(0, blocks, one_block, carried)
        close(dst)

    def through_time(block, vec):
        u = [[[time_ref[0, block, (part * 2 + row) * 3 + c].reshape(planes, rows, LANES) for c in range(3)]
              for row in range(2)] for part in range(2)]
        third = [[], []]
        for c in range(3):
            d, e = (c + 1) % 3, (c + 2) % 3
            third[0].append(u[0][0][d] * u[0][1][e] - u[1][0][d] * u[1][1][e]
                            - u[0][0][e] * u[0][1][d] + u[1][0][e] * u[1][1][d])
            third[1].append(-(u[0][0][d] * u[1][1][e] + u[1][0][d] * u[0][1][e]
                              - u[0][0][e] * u[1][1][d] - u[1][0][e] * u[0][1][d]))
        u[0].append(third[0])
        u[1].append(third[1])
        real, imag = [], []
        for c in range(3):
            real.append(sum(u[0][row][c] * vec[0][row] + u[1][row][c] * vec[1][row] for row in range(3)))
            imag.append(sum(u[0][row][c] * vec[1][row] - u[1][row][c] * vec[0][row] for row in range(3)))
        return [real, imag]

    @pl.when(rounds == 0)
    def _():
        for block in range(blocks):
            for at in range(6):
                value = source_ref[0, block, at].astype(jnp.float32)
                field[at, pl.ds(block * planes, planes)] = value.reshape(planes, rows, LANES)
        close(field)

    hop(field, turned, through_time)
    hop(turned, field, lambda block, vec: vec)
    mine = place_ref[0] * planes
    for at in range(6):
        value = field[at, pl.ds(mine, planes)].reshape(planes * rows, LANES)
        out_ref[0, 0, at] = value.astype(jnp.bfloat16)


def evolve(gauge_all, time_all, sources, starts, place, weights, n_time):
    held, blocks = sources.shape[0], sources.shape[1]
    tile = sources.shape[3]
    planes = evolve.planes
    rows = tile // planes
    side = math.isqrt(rows * LANES)

    def at_time(v, r, start, place):
        return (lax.rem(start[v] + r, n_time), 0, 0, 0, 0)

    kernel = lambda *refs: evolve_kernel(planes, rows, blocks, side, *refs)
    extent = planes * blocks
    return pl.pallas_call(
        kernel,
        out_shape=jax.ShapeDtypeStruct((held, n_time, 6, tile, LANES), jnp.bfloat16),
        grid_spec=pltpu.PrefetchScalarGridSpec(
            num_scalar_prefetch=2,
            grid=(held, n_time),
            in_specs=[
                pl.BlockSpec(memory_space=pltpu.SMEM),
                pl.BlockSpec((1,) + gauge_all.shape[1:], at_time),
                pl.BlockSpec((1,) + time_all.shape[1:], at_time),
                pl.BlockSpec((1,) + sources.shape[1:], lambda v, r, start, place: (v, 0, 0, 0, 0)),
            ],
            out_specs=pl.BlockSpec(
                (1, 1, 6, tile, LANES),
                lambda v, r, start, place: (v, lax.rem(start[v] + r, n_time), 0, 0, 0)),
            scratch_shapes=[pltpu.VMEM((6, extent + 1, rows, LANES), jnp.float32)] * 2,
        ),
        name="evolve",
    )(starts, place, weights, gauge_all, time_all, sources)


def project(sinks, rounded):
    def dot(a, b):
        return jnp.einsum("ecxs,vcxs->ve", a, b, preferred_element_type=jnp.float32)

    real_part = dot(sinks[0], rounded[:, 0]) + dot(sinks[1], rounded[:, 1])
    imag_part = dot(sinks[0], rounded[:, 1]) - dot(sinks[1], rounded[:, 0])
    return jnp.stack([real_part, imag_part])


def local(gauge_links, time_links, sink_vectors, source_times, source_index, kinetic_coef):
    planes, sites = gauge_links.shape[5:]
    tile = planes * sites // LANES
    n_time = lax.axis_size("tm")
    blocks = lax.axis_size("space")
    my_time = lax.axis_index("tm")
    groups, per_group = kinetic_coef.shape
    count = groups * per_group
    held = -(-count // n_time)
    fill = (0, held * n_time - count)
    start_flat = jnp.pad(jnp.repeat(source_times, per_group), fill)
    index_flat = jnp.pad(source_index.reshape(-1), fill)
    coef_flat = jnp.pad(kinetic_coef.reshape(-1), fill)
    my_sinks = sink_vectors[0]

    def gather(x):
        whole = lax.all_gather(x, ("tm", "space"), axis=0, tiled=False)
        return whole.reshape((n_time, blocks) + x.shape)

    gauge_all = gather(gauge_links.astype(jnp.bfloat16).reshape(54, tile, LANES))
    time_all = gather(time_links[0, :, :2].reshape(12, tile, LANES))

    mine = lambda x: lax.dynamic_slice_in_dim(x, my_time * held, held)
    starts = mine(start_flat)
    picked = jnp.take(my_sinks, index_flat, axis=1)
    picked = jnp.moveaxis(picked, 1, 0).reshape(n_time, held, 6, tile, LANES)
    sent = lax.all_to_all(picked, "tm", 0, 0, tiled=False)
    chosen = jnp.stack([lax.dynamic_index_in_dim(sent[:, v], starts[v], 0, keepdims=False)
                        for v in range(held)])
    sources = jnp.moveaxis(lax.all_gather(chosen, "space", axis=0, tiled=False), 0, 1)

    evolve.planes = planes
    place = lax.axis_index("space").astype(jnp.int32)[None]
    evolved = evolve(gauge_all, time_all, sources, starts, place, 0.5 * mine(coef_flat), n_time)
    back = lax.all_to_all(jnp.moveaxis(evolved, 1, 0), "tm", 0, 0, tiled=False)
    rounded = back.reshape(n_time * held, 2, 3, planes, sites)[:count]
    correlations = project(my_sinks, rounded)
    correlations = correlations.reshape(2, groups, per_group, 1, my_sinks.shape[1])
    return lax.psum_scatter(correlations, "space", scatter_dimension=4, tiled=True)


def solution(mesh):
    placed = (
        P("tm", None, None, None, None, "space", None),
        P("tm", None, None, None, "space", None),
        P("tm", None, None, None, "space", None),
        P(),
        P(),
        P(),
    )
    return jax.shard_map(
        local,
        mesh=mesh,
        in_specs=placed,
        out_specs=P(None, None, None, "tm", "space"),
        check_vma=False,
    )
```

```python
import math

import jax
import jax.numpy as jnp
from jax import lax
from jax.experimental import pallas as pl
from jax.experimental.pallas import tpu as pltpu
from jax.sharding import PartitionSpec as P

LANES = 128
MESH = pl.DeviceIdType.MESH


def roll(x, by, axis):
    size = x.shape[axis]
    return pltpu.roll(x, by % size, axis)


def apply_link(link, vec):
    real, imag = [], []
    for a in range(3):
        re = im = None
        for b in range(3):
            ur, ui = link(0, a, b), link(1, a, b)
            r = ur * vec[0][b] - ui * vec[1][b]
            i = ur * vec[1][b] + ui * vec[0][b]
            re = r if re is None else re + r
            im = i if im is None else im + i
        real.append(re)
        imag.append(im)
    return [real, imag]


def apply_both(link, vec_up, vec_here):
    up = [[None] * 3, [None] * 3]
    down = [[None] * 3, [None] * 3]

    def add(out, part, at, value):
        out[part][at] = value if out[part][at] is None else out[part][at] + value

    for a in range(3):
        for b in range(3):
            ur, ui = link(0, a, b), link(1, a, b)
            add(up, 0, a, ur * vec_up[0][b] - ui * vec_up[1][b])
            add(up, 1, a, ur * vec_up[1][b] + ui * vec_up[0][b])
            add(down, 0, b, ur * vec_here[0][a] + ui * vec_here[1][a])
            add(down, 1, b, ur * vec_here[1][a] - ui * vec_here[0][a])
    return up, down


def spread_kernel(n_time, blocks, held, start_ref, gauge_ref, time_ref, picked_ref, gauge_all, time_all,
                  source_all, arrived, chosen, settled, send_sem, recv_sem, self_sem,
                  pick_send, pick_recv, source_send, source_recv):
    t, z = lax.axis_index("tm"), lax.axis_index("space")
    chip, core = t // 2, lax.rem(t, 2)
    chips = n_time // 2
    partner = t + 1 - 2 * core

    barrier = pltpu.get_barrier_semaphore()
    for k in range(1, n_time):
        pl.semaphore_signal(barrier, inc=1, device_id={"tm": lax.rem(t + k, n_time)}, device_id_type=MESH)
    for k in range(1, blocks):
        pl.semaphore_signal(barrier, inc=1, device_id={"space": lax.rem(z + k, blocks)}, device_id_type=MESH)
    pl.semaphore_wait(barrier, n_time + blocks - 2)

    pending = []

    def send(src, dst, send_at, recv_at, target):
        copy = pltpu.make_async_remote_copy(src_ref=src, dst_ref=dst, send_sem=send_at, recv_sem=recv_at,
                                            device_id=target, device_id_type=MESH)
        copy.start()
        pending.append(copy)

    count = [0]

    def send_block(block, target, own=False):
        for kind, (mine, whole) in enumerate(((gauge_ref, gauge_all), (time_ref, time_all))):
            send(mine if own else whole.at[block], whole.at[block], send_sem.at[kind, count[0]],
                 recv_sem.at[kind, block], target)
        count[0] += 1

    def await_block(block):
        for kind, whole in enumerate((gauge_all, time_all)):
            pltpu.make_async_copy(whole.at[block], whole.at[block], recv_sem.at[kind, block]).wait()

    def at(k, of_chip, of_core):
        return (of_chip * 2 + of_core) * blocks + lax.rem(z + k, blocks)

    own = at(0, chip, core)
    square = chips == 4
    if square:
        low, high = lax.rem(chip, 2), chip // 2
        across = chip + 1 - 2 * low
        along = chip + 2 - 4 * high
        corner = 3 - chip
        near = [across, along]
    else:
        near = [lax.rem(chip + k, chips) for k in range(1, chips)]

    def to_chip(of_chip):
        return {"tm": of_chip * 2 + core}

    for k in range(1, blocks):
        send_block(own, {"space": lax.rem(z + k, blocks)}, True)
    for of_chip in near:
        send_block(own, to_chip(of_chip), True)
    locals_ = [pltpu.make_async_copy(gauge_ref, gauge_all.at[own], self_sem.at[0]),
               pltpu.make_async_copy(time_ref, time_all.at[own], self_sem.at[1]),
               pltpu.make_async_copy(picked_ref.at[t], arrived.at[t], self_sem.at[2])]
    for copy in locals_:
        copy.start()
    for k in range(1, n_time):
        to = lax.rem(t + k, n_time)
        send(picked_ref.at[to], arrived.at[t], pick_send.at[k], pick_recv.at[t], {"tm": to})
    send_block(own, {"tm": partner}, True)

    for copy in locals_:
        copy.wait()
    for k in range(1, n_time):
        frm = lax.rem(t + k, n_time)
        pltpu.make_async_copy(arrived.at[frm], arrived.at[frm], pick_recv.at[frm]).wait()
    for v in range(held):
        total = jnp.zeros(arrived.shape[2:], jnp.float32)
        for s in range(n_time):
            flag = jnp.where(start_ref[v] == s, 1.0, 0.0).astype(jnp.float32)
            total = total + flag * arrived[s, v].astype(jnp.float32)
        chosen[v] = total.astype(jnp.bfloat16)
    copy = pltpu.make_async_copy(chosen, settled, self_sem.at[3])
    copy.start()
    copy.wait()
    copy = pltpu.make_async_copy(settled, source_all.at[z], self_sem.at[4])
    copy.start()
    for k in range(1, blocks):
        send(settled, source_all.at[z], source_send.at[k], source_recv.at[z],
             {"space": lax.rem(z + k, blocks)})
    copy.wait()

    order = sorted(range(blocks), key=lambda k: (min(k, blocks - k), k))
    for k in order:
        if k > 0:
            block = at(k, chip, core)
            await_block(block)
            for of_chip in near:
                send_block(block, to_chip(of_chip))
            send_block(block, {"tm": partner})
        for place, of_chip in enumerate(near):
            block = at(k, of_chip, core)
            await_block(block)
            if square and k % 2 == place:
                send_block(block, to_chip(near[1 - place]))
            send_block(block, {"tm": partner})
    if square:
        for k in order:
            block = at(k, corner, core)
            await_block(block)
            send_block(block, {"tm": partner})
    for of_chip in range(chips):
        for k in range(blocks):
            await_block(at(k, of_chip, 1 - core))
    for k in range(1, blocks):
        frm = lax.rem(z + k, blocks)
        pltpu.make_async_copy(source_all.at[frm], source_all.at[frm], source_recv.at[frm]).wait()
    for copy in pending:
        copy.wait_send()


def spread(gauge, time, picked, starts, n_time, blocks):
    held = picked.shape[1]
    n = n_time * blocks
    vmem = pl.BlockSpec(memory_space=pltpu.VMEM)
    anywhere = pl.BlockSpec(memory_space=pl.ANY)
    dma = pltpu.SemaphoreType.DMA
    return pl.pallas_call(
        lambda *refs: spread_kernel(n_time, blocks, held, *refs),
        out_shape=[
            jax.ShapeDtypeStruct((n,) + gauge.shape, gauge.dtype),
            jax.ShapeDtypeStruct((n,) + time.shape, time.dtype),
            jax.ShapeDtypeStruct((blocks,) + picked.shape[1:], picked.dtype),
        ],
        in_specs=[pl.BlockSpec(memory_space=pltpu.SMEM), vmem, vmem, vmem],
        out_specs=[anywhere] * 3,
        scratch_shapes=[
            pltpu.VMEM(picked.shape, picked.dtype),
            pltpu.VMEM(picked.shape[1:], picked.dtype),
            pltpu.VMEM(picked.shape[1:], picked.dtype),
            dma((2, n + blocks + n)), dma((2, n)), dma((5,)),
            dma((n_time,)), dma((n_time,)), dma((blocks,)), dma((blocks,)),
        ],
        compiler_params=pltpu.CompilerParams(collective_id=0, has_side_effects=True),
        name="spread",
    )(starts, gauge, time, picked)


def evolve_kernel(planes, rows, blocks, side, start_ref, place_ref, weight_ref, gauge_ref, time_ref,
                  source_ref, out_ref, field, turned, wide):
    which, rounds = pl.program_id(0), pl.program_id(1)
    extent = planes * blocks
    weight = weight_ref[which]
    lane = lax.broadcasted_iota(jnp.int32, (planes, rows, LANES), 2)
    per_row = LANES // side

    def y_up(x):
        turned_lanes = roll(x, -side, 2)
        return jnp.where(lane < LANES - side, turned_lanes, roll(turned_lanes, -1, 1))

    def y_down(x):
        turned_lanes = roll(x, side, 2)
        return jnp.where(lane >= side, turned_lanes, roll(turned_lanes, 1, 1))

    def z_up(x):
        return jnp.where(lane % side == side - 1, roll(x, side - 1, 2), roll(x, -1, 2))

    def z_down(x):
        return jnp.where(lane % side == 0, roll(x, 1 - side, 2), roll(x, 1, 2))

    def gauge(block, direction):
        def link(part, row, column):
            return wide[block, ((part * 3 + direction) * 3 + row) * 3 + column]
        return link

    def shaped(x):
        return x.astype(jnp.float32).reshape(planes, rows, LANES)

    def third_row(u):
        real, imag = [], []
        for c in range(3):
            d, e = (c + 1) % 3, (c + 2) % 3
            real.append(u[0][0][d] * u[0][1][e] - u[1][0][d] * u[1][1][e]
                        - u[0][0][e] * u[0][1][d] + u[1][0][e] * u[1][1][d])
            imag.append(u[0][0][e] * u[1][1][d] + u[1][0][e] * u[0][1][d]
                        - u[0][0][d] * u[1][1][e] - u[1][0][d] * u[0][1][e])
        return real, imag

    def widen(block, nothing):
        for direction in range(3):
            u = [[[shaped(gauge_ref[0, block, ((part * 3 + direction) * 2 + row) * 3 + c])
                   for c in range(3)] for row in range(2)] for part in range(2)]
            for part, extra in enumerate(third_row(u)):
                for row, values in enumerate(u[part] + [extra]):
                    for c in range(3):
                        wide[block, ((part * 3 + direction) * 3 + row) * 3 + c] = values[c]
        return nothing

    def read(ref, first):
        return [[ref[part * 3 + c, pl.ds(first, planes)] for c in range(3)] for part in range(2)]

    def each(fn, vec):
        return [[fn(vec[part][c]) for c in range(3)] for part in range(2)]

    def plus(*vecs):
        return [[sum(v[part][c] for v in vecs[1:]) + vecs[0][part][c] for c in range(3)] for part in range(2)]

    def close(ref):
        for at in range(6):
            ref[at, pl.ds(extent, 1)] = ref[at, pl.ds(0, 1)]

    def hop(src, dst, then):
        last = read(src, extent - planes)
        _, wrapped = apply_both(gauge(blocks - 1, 0), last, last)
        carried = tuple(wrapped[part][c][planes - 1:] for part in range(2) for c in range(3))

        def one_block(block, carry):
            first = block * planes
            here = read(src, first)
            up, down = apply_both(gauge(block, 0), read(src, first + 1), here)
            flat = [down[part][c] for part in range(2) for c in range(3)]
            moved = [jnp.concatenate([low, x[: planes - 1]], axis=0) for low, x in zip(carry, flat)]
            total = plus(up, [moved[:3], moved[3:]])
            up, down = apply_both(gauge(block, 1), each(y_up, here), here)
            total = plus(total, up, each(y_down, down))
            up, down = apply_both(gauge(block, 2), each(z_up, here), here)
            total = plus(total, up, each(z_down, down))
            result = [[here[part][c] + weight * (total[part][c] - 6.0 * here[part][c]) for c in range(3)]
                      for part in range(2)]
            result = then(block, result)
            for part in range(2):
                for c in range(3):
                    dst[part * 3 + c, pl.ds(first, planes)] = result[part][c]
            return tuple(x[planes - 1:] for x in flat)

        lax.fori_loop(0, blocks, one_block, carried)
        close(dst)

    def through_time(block, vec):
        u = [[[shaped(time_ref[0, block, (part * 2 + row) * 3 + c]) for c in range(3)]
              for row in range(2)] for part in range(2)]
        for part, extra in enumerate(third_row(u)):
            u[part].append(extra)
        real, imag = [], []
        for c in range(3):
            real.append(sum(u[0][row][c] * vec[0][row] + u[1][row][c] * vec[1][row] for row in range(3)))
            imag.append(sum(u[0][row][c] * vec[1][row] - u[1][row][c] * vec[0][row] for row in range(3)))
        return [real, imag]

    @pl.when(rounds == 0)
    def _():
        for block in range(blocks):
            for at in range(6):
                value = source_ref[0, block, at].astype(jnp.float32)
                field[at, pl.ds(block * planes, planes)] = value.reshape(planes, rows, LANES)
        close(field)

    lax.fori_loop(0, blocks, widen, 0)
    hop(field, turned, through_time)
    hop(turned, field, lambda block, vec: vec)
    mine = place_ref[0] * planes
    for at in range(6):
        value = field[at, pl.ds(mine, planes)].reshape(planes * rows, LANES)
        out_ref[0, 0, at] = value.astype(jnp.bfloat16)


def evolve(gauge_all, time_all, sources, starts, place, weights, n_time):
    held, blocks = sources.shape[0], sources.shape[1]
    tile = sources.shape[3]
    planes = evolve.planes
    rows = tile // planes
    side = math.isqrt(rows * LANES)

    def at_time(v, r, start, place):
        return (lax.rem(start[v] + r, n_time), 0, 0, 0, 0)

    kernel = lambda *refs: evolve_kernel(planes, rows, blocks, side, *refs)
    extent = planes * blocks
    return pl.pallas_call(
        kernel,
        out_shape=jax.ShapeDtypeStruct((held, n_time, 6, tile, LANES), jnp.bfloat16),
        grid_spec=pltpu.PrefetchScalarGridSpec(
            num_scalar_prefetch=2,
            grid=(held, n_time),
            in_specs=[
                pl.BlockSpec(memory_space=pltpu.SMEM),
                pl.BlockSpec((1,) + gauge_all.shape[1:], at_time),
                pl.BlockSpec((1,) + time_all.shape[1:], at_time),
                pl.BlockSpec((1,) + sources.shape[1:], lambda v, r, start, place: (v, 0, 0, 0, 0)),
            ],
            out_specs=pl.BlockSpec(
                (1, 1, 6, tile, LANES),
                lambda v, r, start, place: (v, lax.rem(start[v] + r, n_time), 0, 0, 0)),
            scratch_shapes=[pltpu.VMEM((6, extent + 1, rows, LANES), jnp.float32)] * 2
            + [pltpu.VMEM((blocks, 54, planes, rows, LANES), jnp.float32)],
        ),
        name="evolve",
    )(starts, place, weights, gauge_all, time_all, sources)


def project(sinks, rounded):
    def dot(a, b):
        return jnp.einsum("ecxs,vcxs->ve", a, b, preferred_element_type=jnp.float32)

    real_part = dot(sinks[0], rounded[:, 0]) + dot(sinks[1], rounded[:, 1])
    imag_part = dot(sinks[0], rounded[:, 1]) - dot(sinks[1], rounded[:, 0])
    return jnp.stack([real_part, imag_part])


def local(gauge_links, time_links, sink_vectors, source_times, source_index, kinetic_coef):
    planes, sites = gauge_links.shape[5:]
    tile = planes * sites // LANES
    n_time = lax.axis_size("tm")
    blocks = lax.axis_size("space")
    my_time = lax.axis_index("tm")
    groups, per_group = kinetic_coef.shape
    count = groups * per_group
    held = -(-count // n_time)
    fill = (0, held * n_time - count)
    start_flat = jnp.pad(jnp.repeat(source_times, per_group), fill)
    index_flat = jnp.pad(source_index.reshape(-1), fill)
    coef_flat = jnp.pad(kinetic_coef.reshape(-1), fill)
    my_sinks = sink_vectors[0]

    mine = lambda x: lax.dynamic_slice_in_dim(x, my_time * held, held)
    starts = mine(start_flat)
    gauge = gauge_links[0, :, :, :2].astype(jnp.bfloat16).reshape(36, tile, LANES)
    time = time_links[0, :, :2].reshape(12, tile, LANES)
    picked = jnp.take(my_sinks, index_flat, axis=1)
    picked = jnp.moveaxis(picked, 1, 0).reshape(n_time, held, 6, tile, LANES)
    gauge_all, time_all, sources = spread(gauge, time, picked, starts, n_time, blocks)
    gauge_all = gauge_all.reshape((n_time, blocks) + gauge.shape)
    time_all = time_all.reshape((n_time, blocks) + time.shape)
    sources = jnp.moveaxis(sources, 0, 1)

    evolve.planes = planes
    place = lax.axis_index("space").astype(jnp.int32)[None]
    evolved = evolve(gauge_all, time_all, sources, starts, place, 0.5 * mine(coef_flat), n_time)
    back = lax.all_to_all(jnp.moveaxis(evolved, 1, 0), "tm", 0, 0, tiled=False)
    rounded = back.reshape(n_time * held, 2, 3, planes, sites)[:count]
    correlations = project(my_sinks, rounded)
    correlations = correlations.reshape(2, groups, per_group, 1, my_sinks.shape[1])
    return lax.psum_scatter(correlations, "space", scatter_dimension=4, tiled=True)


def solution(mesh):
    placed = (
        P("tm", None, None, None, None, "space", None),
        P("tm", None, None, None, "space", None),
        P("tm", None, None, None, "space", None),
        P(),
        P(),
        P(),
    )
    return jax.shard_map(
        local,
        mesh=mesh,
        in_specs=placed,
        out_specs=P(None, None, None, "tm", "space"),
        check_vma=False,
    )
```

```python
import math

import jax
import jax.numpy as jnp
from jax import lax
from jax.experimental import pallas as pl
from jax.experimental.pallas import tpu as pltpu
from jax.sharding import PartitionSpec as P

LANES = 128
MESH = pl.DeviceIdType.MESH


def roll(x, by, axis):
    size = x.shape[axis]
    return pltpu.roll(x, by % size, axis)


def apply_link(link, vec):
    real, imag = [], []
    for a in range(3):
        re = im = None
        for b in range(3):
            ur, ui = link(0, a, b), link(1, a, b)
            r = ur * vec[0][b] - ui * vec[1][b]
            i = ur * vec[1][b] + ui * vec[0][b]
            re = r if re is None else re + r
            im = i if im is None else im + i
        real.append(re)
        imag.append(im)
    return [real, imag]


def apply_both(link, vec_up, vec_here):
    up = [[None] * 3, [None] * 3]
    down = [[None] * 3, [None] * 3]

    def add(out, part, at, value):
        out[part][at] = value if out[part][at] is None else out[part][at] + value

    for a in range(3):
        for b in range(3):
            ur, ui = link(0, a, b), link(1, a, b)
            add(up, 0, a, ur * vec_up[0][b] - ui * vec_up[1][b])
            add(up, 1, a, ur * vec_up[1][b] + ui * vec_up[0][b])
            add(down, 0, b, ur * vec_here[0][a] + ui * vec_here[1][a])
            add(down, 1, b, ur * vec_here[1][a] - ui * vec_here[0][a])
    return up, down


def spread_kernel(n_time, blocks, held, start_ref, gauge_ref, time_ref, picked_ref, gauge_all, time_all,
                  source_all, arrived, chosen, settled, send_sem, recv_sem, self_sem,
                  pick_send, pick_recv, source_send, source_recv):
    t, z = lax.axis_index("tm"), lax.axis_index("space")
    chip, core = t // 2, lax.rem(t, 2)
    chips = n_time // 2
    partner = t + 1 - 2 * core

    barrier = pltpu.get_barrier_semaphore()
    for k in range(1, n_time):
        pl.semaphore_signal(barrier, inc=1, device_id={"tm": lax.rem(t + k, n_time)}, device_id_type=MESH)
    for k in range(1, blocks):
        pl.semaphore_signal(barrier, inc=1, device_id={"space": lax.rem(z + k, blocks)}, device_id_type=MESH)
    pl.semaphore_wait(barrier, n_time + blocks - 2)

    pending = []

    def when(condition, action):
        if condition is None:
            action()
        else:
            pl.when(condition)(action)

    def both(first, second):
        return second if first is None else first if second is None else jnp.logical_and(first, second)

    def send(src, dst, send_at, recv_at, target, condition=None):
        copy = pltpu.make_async_remote_copy(src_ref=src, dst_ref=dst, send_sem=send_at, recv_sem=recv_at,
                                            device_id=target, device_id_type=MESH)
        when(condition, copy.start)
        pending.append((condition, copy))

    count = [0]

    def send_block(block, target, condition=None, own=False):
        for kind, (mine, whole) in enumerate(((gauge_ref, gauge_all), (time_ref, time_all))):
            send(mine if own else whole.at[block], whole.at[block], send_sem.at[kind, count[0]],
                 recv_sem.at[kind, block], target, condition)
        count[0] += 1

    def await_block(block, condition=None):
        def wait():
            for kind, whole in enumerate((gauge_all, time_all)):
                pltpu.make_async_copy(whole.at[block], whole.at[block], recv_sem.at[kind, block]).wait()
        when(condition, wait)

    def at(depth, of_chip, of_core):
        return (of_chip * 2 + of_core) * blocks + depth

    own = at(z, chip, core)
    square = chips == 4
    if square:
        low, high = lax.rem(chip, 2), chip // 2
        across = chip + 1 - 2 * low
        along = chip + 2 - 4 * high
        corner = 3 - chip
        near = [across, along]
    else:
        near = [lax.rem(chip + k, chips) for k in range(1, chips)]

    def to_chip(of_chip):
        return {"tm": of_chip * 2 + core}

    below = (z > 0, {"space": lax.rem(z + blocks - 1, blocks)})
    above = (z < blocks - 1, {"space": lax.rem(z + 1, blocks)})
    for condition, target in (below, above):
        send_block(own, target, condition, True)
    for k in range(1, n_time):
        to = lax.rem(t + k, n_time)
        send(picked_ref.at[to], arrived.at[t], pick_send.at[k], pick_recv.at[t], {"tm": to})
    for of_chip in near:
        send_block(own, to_chip(of_chip), None, True)
    send_block(own, {"tm": partner}, None, True)
    locals_ = [pltpu.make_async_copy(gauge_ref, gauge_all.at[own], self_sem.at[0]),
               pltpu.make_async_copy(time_ref, time_all.at[own], self_sem.at[1]),
               pltpu.make_async_copy(picked_ref.at[t], arrived.at[t], self_sem.at[2])]
    for copy in locals_:
        copy.start()
    def settle():
        for copy in locals_:
            copy.wait()
        for k in range(1, n_time):
            frm = lax.rem(t + k, n_time)
            pltpu.make_async_copy(arrived.at[frm], arrived.at[frm], pick_recv.at[frm]).wait()
        for v in range(held):
            total = jnp.zeros(arrived.shape[2:], jnp.float32)
            for s in range(n_time):
                flag = jnp.where(start_ref[v] == s, 1.0, 0.0).astype(jnp.float32)
                total = total + flag * arrived[s, v].astype(jnp.float32)
            chosen[v] = total.astype(jnp.bfloat16)
        copy = pltpu.make_async_copy(chosen, settled, self_sem.at[3])
        copy.start()
        copy.wait()
        copy = pltpu.make_async_copy(settled, source_all.at[z], self_sem.at[4])
        copy.start()
        for k in range(1, blocks):
            send(settled, source_all.at[z], source_send.at[k], source_recv.at[z],
                 {"space": lax.rem(z + k, blocks)})
        copy.wait()

    items = [(0, None, z, None)]
    for step in range(1, blocks):
        items.append((step, z >= step, lax.rem(z + blocks - step, blocks), above))
        items.append((step, z + step < blocks, lax.rem(z + step, blocks), below))

    def from_column(item):
        step, condition, depth, onward = item
        block = at(depth, chip, core)
        await_block(block, condition)
        send_block(block, onward[1], both(condition, onward[0]))
        for of_chip in near:
            send_block(block, to_chip(of_chip), condition)
        send_block(block, {"tm": partner}, condition)

    def from_near(item):
        step, condition, depth, onward = item
        for place, of_chip in enumerate(near):
            block = at(depth, of_chip, core)
            await_block(block, condition)
            if square and step % 2 == place:
                send_block(block, to_chip(near[1 - place]), condition)
            send_block(block, {"tm": partner}, condition)

    for place, item in enumerate(items):
        if place > 0:
            from_column(item)
            from_near(items[place - 1])
        if place == min(2, len(items) - 1):
            settle()
    from_near(items[-1])
    if square:
        for step, condition, depth, onward in items:
            block = at(depth, corner, core)
            await_block(block, condition)
            send_block(block, {"tm": partner}, condition)
    for of_chip in range(chips):
        for depth in range(blocks):
            await_block(at(depth, of_chip, 1 - core))
    for k in range(1, blocks):
        frm = lax.rem(z + k, blocks)
        pltpu.make_async_copy(source_all.at[frm], source_all.at[frm], source_recv.at[frm]).wait()
    for condition, copy in pending:
        when(condition, copy.wait_send)


def spread(gauge, time, picked, starts, n_time, blocks):
    held = picked.shape[1]
    n = n_time * blocks
    vmem = pl.BlockSpec(memory_space=pltpu.VMEM)
    anywhere = pl.BlockSpec(memory_space=pl.ANY)
    dma = pltpu.SemaphoreType.DMA
    return pl.pallas_call(
        lambda *refs: spread_kernel(n_time, blocks, held, *refs),
        out_shape=[
            jax.ShapeDtypeStruct((n,) + gauge.shape, gauge.dtype),
            jax.ShapeDtypeStruct((n,) + time.shape, time.dtype),
            jax.ShapeDtypeStruct((blocks,) + picked.shape[1:], picked.dtype),
        ],
        in_specs=[pl.BlockSpec(memory_space=pltpu.SMEM), vmem, vmem, vmem],
        out_specs=[anywhere] * 3,
        scratch_shapes=[
            pltpu.VMEM(picked.shape, picked.dtype),
            pltpu.VMEM(picked.shape[1:], picked.dtype),
            pltpu.VMEM(picked.shape[1:], picked.dtype),
            dma((2, 4 * n + 8)), dma((2, n)), dma((5,)),
            dma((n_time,)), dma((n_time,)), dma((blocks,)), dma((blocks,)),
        ],
        compiler_params=pltpu.CompilerParams(collective_id=0, has_side_effects=True),
        name="spread",
    )(starts, gauge, time, picked)


def evolve_kernel(planes, rows, blocks, side, start_ref, place_ref, weight_ref, gauge_ref, time_ref,
                  source_ref, out_ref, field, turned, wide):
    which, rounds = pl.program_id(0), pl.program_id(1)
    extent = planes * blocks
    weight = weight_ref[which]
    lane = lax.broadcasted_iota(jnp.int32, (planes, rows, LANES), 2)
    per_row = LANES // side

    def y_up(x):
        turned_lanes = roll(x, -side, 2)
        return jnp.where(lane < LANES - side, turned_lanes, roll(turned_lanes, -1, 1))

    def y_down(x):
        turned_lanes = roll(x, side, 2)
        return jnp.where(lane >= side, turned_lanes, roll(turned_lanes, 1, 1))

    def z_up(x):
        return jnp.where(lane % side == side - 1, roll(x, side - 1, 2), roll(x, -1, 2))

    def z_down(x):
        return jnp.where(lane % side == 0, roll(x, 1 - side, 2), roll(x, 1, 2))

    def gauge(block, direction):
        def link(part, row, column):
            return wide[block, ((part * 3 + direction) * 3 + row) * 3 + column]
        return link

    def shaped(x):
        return x.astype(jnp.float32).reshape(planes, rows, LANES)

    def third_row(u):
        real, imag = [], []
        for c in range(3):
            d, e = (c + 1) % 3, (c + 2) % 3
            real.append(u[0][0][d] * u[0][1][e] - u[1][0][d] * u[1][1][e]
                        - u[0][0][e] * u[0][1][d] + u[1][0][e] * u[1][1][d])
            imag.append(u[0][0][e] * u[1][1][d] + u[1][0][e] * u[0][1][d]
                        - u[0][0][d] * u[1][1][e] - u[1][0][d] * u[0][1][e])
        return real, imag

    def widen(block, nothing):
        for direction in range(3):
            u = [[[shaped(gauge_ref[0, block, ((part * 3 + direction) * 2 + row) * 3 + c])
                   for c in range(3)] for row in range(2)] for part in range(2)]
            for part, extra in enumerate(third_row(u)):
                for row, values in enumerate(u[part] + [extra]):
                    for c in range(3):
                        wide[block, ((part * 3 + direction) * 3 + row) * 3 + c] = values[c]
        return nothing

    def read(ref, first):
        return [[ref[part * 3 + c, pl.ds(first, planes)] for c in range(3)] for part in range(2)]

    def each(fn, vec):
        return [[fn(vec[part][c]) for c in range(3)] for part in range(2)]

    def plus(*vecs):
        return [[sum(v[part][c] for v in vecs[1:]) + vecs[0][part][c] for c in range(3)] for part in range(2)]

    def close(ref):
        for at in range(6):
            ref[at, pl.ds(extent, 1)] = ref[at, pl.ds(0, 1)]

    def hop(src, dst, then):
        last = read(src, extent - planes)
        _, wrapped = apply_both(gauge(blocks - 1, 0), last, last)
        carried = tuple(wrapped[part][c][planes - 1:] for part in range(2) for c in range(3))

        def one_block(block, carry):
            first = block * planes
            here = read(src, first)
            up, down = apply_both(gauge(block, 0), read(src, first + 1), here)
            flat = [down[part][c] for part in range(2) for c in range(3)]
            moved = [jnp.concatenate([low, x[: planes - 1]], axis=0) for low, x in zip(carry, flat)]
            total = plus(up, [moved[:3], moved[3:]])
            up, down = apply_both(gauge(block, 1), each(y_up, here), here)
            total = plus(total, up, each(y_down, down))
            up, down = apply_both(gauge(block, 2), each(z_up, here), here)
            total = plus(total, up, each(z_down, down))
            result = [[here[part][c] + weight * (total[part][c] - 6.0 * here[part][c]) for c in range(3)]
                      for part in range(2)]
            result = then(block, result)
            for part in range(2):
                for c in range(3):
                    dst[part * 3 + c, pl.ds(first, planes)] = result[part][c]
            return tuple(x[planes - 1:] for x in flat)

        lax.fori_loop(0, blocks, one_block, carried)
        close(dst)

    def through_time(block, vec):
        u = [[[shaped(time_ref[0, block, (part * 2 + row) * 3 + c]) for c in range(3)]
              for row in range(2)] for part in range(2)]
        for part, extra in enumerate(third_row(u)):
            u[part].append(extra)
        real, imag = [], []
        for c in range(3):
            real.append(sum(u[0][row][c] * vec[0][row] + u[1][row][c] * vec[1][row] for row in range(3)))
            imag.append(sum(u[0][row][c] * vec[1][row] - u[1][row][c] * vec[0][row] for row in range(3)))
        return [real, imag]

    @pl.when(rounds == 0)
    def _():
        for block in range(blocks):
            for at in range(6):
                value = source_ref[0, block, at].astype(jnp.float32)
                field[at, pl.ds(block * planes, planes)] = value.reshape(planes, rows, LANES)
        close(field)

    lax.fori_loop(0, blocks, widen, 0)
    hop(field, turned, through_time)
    hop(turned, field, lambda block, vec: vec)
    mine = place_ref[0] * planes
    for at in range(6):
        value = field[at, pl.ds(mine, planes)].reshape(planes * rows, LANES)
        out_ref[0, 0, at] = value.astype(jnp.bfloat16)


def evolve(gauge_all, time_all, sources, starts, place, weights, n_time):
    held, blocks = sources.shape[0], sources.shape[1]
    tile = sources.shape[3]
    planes = evolve.planes
    rows = tile // planes
    side = math.isqrt(rows * LANES)

    def at_time(v, r, start, place):
        return (lax.rem(start[v] + r, n_time), 0, 0, 0, 0)

    kernel = lambda *refs: evolve_kernel(planes, rows, blocks, side, *refs)
    extent = planes * blocks
    return pl.pallas_call(
        kernel,
        out_shape=jax.ShapeDtypeStruct((held, n_time, 6, tile, LANES), jnp.bfloat16),
        grid_spec=pltpu.PrefetchScalarGridSpec(
            num_scalar_prefetch=2,
            grid=(held, n_time),
            in_specs=[
                pl.BlockSpec(memory_space=pltpu.SMEM),
                pl.BlockSpec((1,) + gauge_all.shape[1:], at_time),
                pl.BlockSpec((1,) + time_all.shape[1:], at_time),
                pl.BlockSpec((1,) + sources.shape[1:], lambda v, r, start, place: (v, 0, 0, 0, 0)),
            ],
            out_specs=pl.BlockSpec(
                (1, 1, 6, tile, LANES),
                lambda v, r, start, place: (v, lax.rem(start[v] + r, n_time), 0, 0, 0)),
            scratch_shapes=[pltpu.VMEM((6, extent + 1, rows, LANES), jnp.float32)] * 2
            + [pltpu.VMEM((blocks, 54, planes, rows, LANES), jnp.float32)],
        ),
        name="evolve",
    )(starts, place, weights, gauge_all, time_all, sources)


def collect_kernel(blocks, part_ref, out_ref, parts, send_sem, recv_sem, self_sem):
    z = lax.axis_index("space")
    barrier = pltpu.get_barrier_semaphore()
    others = [lax.rem(z + k, blocks) for k in range(1, blocks)]
    for other in others:
        pl.semaphore_signal(barrier, inc=1, device_id={"space": other}, device_id_type=MESH)
    pl.semaphore_wait(barrier, blocks - 1)
    copies = []
    for k, other in enumerate(others):
        copies.append(pltpu.make_async_remote_copy(
            src_ref=part_ref, dst_ref=parts.at[z], send_sem=send_sem.at[k], recv_sem=recv_sem.at[z],
            device_id={"space": other}, device_id_type=MESH))
        copies[-1].start()
    mine = pltpu.make_async_copy(part_ref, parts.at[z], self_sem)
    mine.start()
    mine.wait()
    for other in others:
        pltpu.make_async_copy(parts.at[other], parts.at[other], recv_sem.at[other]).wait()
    for copy in copies:
        copy.wait_send()
    total = parts[0]
    for block in range(1, blocks):
        total = total + parts[block]
    width = out_ref.shape[1]
    kept = total[:, :width]
    for block in range(1, blocks):
        kept = jnp.where(z == block, total[:, block * width:(block + 1) * width], kept)
    out_ref[...] = kept


def collect(partial, blocks):
    rows, columns = partial.shape
    vmem = pl.BlockSpec(memory_space=pltpu.VMEM)
    dma = pltpu.SemaphoreType.DMA
    return pl.pallas_call(
        lambda *refs: collect_kernel(blocks, *refs),
        out_shape=jax.ShapeDtypeStruct((rows, columns // blocks), jnp.float32),
        in_specs=[vmem],
        out_specs=vmem,
        scratch_shapes=[pltpu.VMEM((blocks, rows, columns), jnp.float32),
                        dma((blocks,)), dma((blocks,)), dma],
        compiler_params=pltpu.CompilerParams(collective_id=1, has_side_effects=True),
        name="collect",
    )(partial)


def project(sinks, rounded):
    def dot(a, b):
        return jnp.einsum("ecxs,vcxs->ve", a, b, preferred_element_type=jnp.float32)

    real_part = dot(sinks[0], rounded[:, 0]) + dot(sinks[1], rounded[:, 1])
    imag_part = dot(sinks[0], rounded[:, 1]) - dot(sinks[1], rounded[:, 0])
    return jnp.stack([real_part, imag_part])


def local(gauge_links, time_links, sink_vectors, source_times, source_index, kinetic_coef):
    planes, sites = gauge_links.shape[5:]
    tile = planes * sites // LANES
    n_time = lax.axis_size("tm")
    blocks = lax.axis_size("space")
    my_time = lax.axis_index("tm")
    groups, per_group = kinetic_coef.shape
    count = groups * per_group
    held = -(-count // n_time)
    fill = (0, held * n_time - count)
    start_flat = jnp.pad(jnp.repeat(source_times, per_group), fill)
    index_flat = jnp.pad(source_index.reshape(-1), fill)
    coef_flat = jnp.pad(kinetic_coef.reshape(-1), fill)
    my_sinks = sink_vectors[0]

    mine = lambda x: lax.dynamic_slice_in_dim(x, my_time * held, held)
    starts = mine(start_flat)
    gauge = gauge_links[0, :, :, :2].astype(jnp.bfloat16).reshape(36, tile, LANES)
    time = time_links[0, :, :2].reshape(12, tile, LANES)
    picked = jnp.take(my_sinks, index_flat, axis=1)
    picked = jnp.moveaxis(picked, 1, 0).reshape(n_time, held, 6, tile, LANES)
    gauge_all, time_all, sources = spread(gauge, time, picked, starts, n_time, blocks)
    gauge_all = gauge_all.reshape((n_time, blocks) + gauge.shape)
    time_all = time_all.reshape((n_time, blocks) + time.shape)
    sources = jnp.moveaxis(sources, 0, 1)

    evolve.planes = planes
    place = lax.axis_index("space").astype(jnp.int32)[None]
    evolved = evolve(gauge_all, time_all, sources, starts, place, 0.5 * mine(coef_flat), n_time)
    back = lax.all_to_all(jnp.moveaxis(evolved, 1, 0), "tm", 0, 0, tiled=False)
    rounded = back.reshape(n_time * held, 2, 3, planes, sites)[:count]
    correlations = project(my_sinks, rounded)
    total = collect(correlations.reshape(2 * count, -1), blocks)
    return total.reshape(2, groups, per_group, 1, -1)


def solution(mesh):
    placed = (
        P("tm", None, None, None, None, "space", None),
        P("tm", None, None, None, "space", None),
        P("tm", None, None, None, "space", None),
        P(),
        P(),
        P(),
    )
    return jax.shard_map(
        local,
        mesh=mesh,
        in_specs=placed,
        out_specs=P(None, None, None, "tm", "space"),
        check_vma=False,
    )
```

```python
import math

import jax
import jax.numpy as jnp
from jax import lax
from jax.experimental import pallas as pl
from jax.experimental.pallas import tpu as pltpu
from jax.sharding import PartitionSpec as P

LANES = 128
MESH = pl.DeviceIdType.MESH
VMEM_ROOM = 24 * 1024 * 1024


def roll(x, by, axis):
    size = x.shape[axis]
    return pltpu.roll(x, by % size, axis)


def apply_link(link, vec):
    real, imag = [], []
    for a in range(3):
        re = im = None
        for b in range(3):
            ur, ui = link(0, a, b), link(1, a, b)
            r = ur * vec[0][b] - ui * vec[1][b]
            i = ur * vec[1][b] + ui * vec[0][b]
            re = r if re is None else re + r
            im = i if im is None else im + i
        real.append(re)
        imag.append(im)
    return [real, imag]


def apply_both(link, vec_up, vec_here):
    up = [[None] * 3, [None] * 3]
    down = [[None] * 3, [None] * 3]

    def add(out, part, at, value):
        out[part][at] = value if out[part][at] is None else out[part][at] + value

    for a in range(3):
        for b in range(3):
            ur, ui = link(0, a, b), link(1, a, b)
            add(up, 0, a, ur * vec_up[0][b] - ui * vec_up[1][b])
            add(up, 1, a, ur * vec_up[1][b] + ui * vec_up[0][b])
            add(down, 0, b, ur * vec_here[0][a] + ui * vec_here[1][a])
            add(down, 1, b, ur * vec_here[1][a] - ui * vec_here[0][a])
    return up, down


def spread_kernel(n_time, blocks, held, start_ref, gauge_ref, time_ref, picked_ref, gauge_all, time_all,
                  source_all, arrived, chosen, settled, send_sem, recv_sem, self_sem,
                  pick_send, pick_recv, source_send, source_recv):
    t, z = lax.axis_index("tm"), lax.axis_index("space")
    chip, core = t // 2, lax.rem(t, 2)
    chips = n_time // 2
    partner = t + 1 - 2 * core

    barrier = pltpu.get_barrier_semaphore()
    for k in range(1, n_time):
        pl.semaphore_signal(barrier, inc=1, device_id={"tm": lax.rem(t + k, n_time)}, device_id_type=MESH)
    for k in range(1, blocks):
        pl.semaphore_signal(barrier, inc=1, device_id={"space": lax.rem(z + k, blocks)}, device_id_type=MESH)
    pl.semaphore_wait(barrier, n_time + blocks - 2)

    pending = []

    def when(condition, action):
        if condition is None:
            action()
        else:
            pl.when(condition)(action)

    def both(first, second):
        return second if first is None else first if second is None else jnp.logical_and(first, second)

    def send(src, dst, send_at, recv_at, target, condition=None):
        copy = pltpu.make_async_remote_copy(src_ref=src, dst_ref=dst, send_sem=send_at, recv_sem=recv_at,
                                            device_id=target, device_id_type=MESH)
        when(condition, copy.start)
        pending.append((condition, copy))

    count = [0]

    def send_block(block, target, condition=None, own=False):
        for kind, (mine, whole) in enumerate(((gauge_ref, gauge_all), (time_ref, time_all))):
            send(mine if own else whole.at[block], whole.at[block], send_sem.at[kind, count[0]],
                 recv_sem.at[kind, block], target, condition)
        count[0] += 1

    def await_block(block, condition=None):
        def wait():
            for kind, whole in enumerate((gauge_all, time_all)):
                pltpu.make_async_copy(whole.at[block], whole.at[block], recv_sem.at[kind, block]).wait()
        when(condition, wait)

    def at(depth, of_chip, of_core):
        return (of_chip * 2 + of_core) * blocks + depth

    own = at(z, chip, core)
    square = chips == 4
    if square:
        low, high = lax.rem(chip, 2), chip // 2
        across = chip + 1 - 2 * low
        along = chip + 2 - 4 * high
        corner = 3 - chip
        near = [across, along]
    else:
        near = [lax.rem(chip + k, chips) for k in range(1, chips)]

    def to_chip(of_chip):
        return {"tm": of_chip * 2 + core}

    below = (z > 0, {"space": lax.rem(z + blocks - 1, blocks)})
    above = (z < blocks - 1, {"space": lax.rem(z + 1, blocks)})
    for condition, target in (below, above):
        send_block(own, target, condition, True)
    for k in range(1, n_time):
        to = lax.rem(t + k, n_time)
        send(picked_ref.at[to], arrived.at[t], pick_send.at[k], pick_recv.at[t], {"tm": to})
    for of_chip in near:
        send_block(own, to_chip(of_chip), None, True)
    send_block(own, {"tm": partner}, None, True)
    locals_ = [pltpu.make_async_copy(gauge_ref, gauge_all.at[own], self_sem.at[0]),
               pltpu.make_async_copy(time_ref, time_all.at[own], self_sem.at[1]),
               pltpu.make_async_copy(picked_ref.at[t], arrived.at[t], self_sem.at[2])]
    for copy in locals_:
        copy.start()
    def settle():
        for copy in locals_:
            copy.wait()
        for k in range(1, n_time):
            frm = lax.rem(t + k, n_time)
            pltpu.make_async_copy(arrived.at[frm], arrived.at[frm], pick_recv.at[frm]).wait()
        for v in range(held):
            total = jnp.zeros(arrived.shape[2:], jnp.float32)
            for s in range(n_time):
                flag = jnp.where(start_ref[v] == s, 1.0, 0.0).astype(jnp.float32)
                total = total + flag * arrived[s, v].astype(jnp.float32)
            chosen[v] = total.astype(jnp.bfloat16)
        copy = pltpu.make_async_copy(chosen, settled, self_sem.at[3])
        copy.start()
        copy.wait()
        copy = pltpu.make_async_copy(settled, source_all.at[z], self_sem.at[4])
        copy.start()
        for k in range(1, blocks):
            send(settled, source_all.at[z], source_send.at[k], source_recv.at[z],
                 {"space": lax.rem(z + k, blocks)})
        copy.wait()

    items = [(0, None, z, None)]
    for step in range(1, blocks):
        items.append((step, z >= step, lax.rem(z + blocks - step, blocks), above))
        items.append((step, z + step < blocks, lax.rem(z + step, blocks), below))

    def from_column(item):
        step, condition, depth, onward = item
        block = at(depth, chip, core)
        await_block(block, condition)
        send_block(block, onward[1], both(condition, onward[0]))
        for of_chip in near:
            send_block(block, to_chip(of_chip), condition)
        send_block(block, {"tm": partner}, condition)

    def from_near(item):
        step, condition, depth, onward = item
        for place, of_chip in enumerate(near):
            block = at(depth, of_chip, core)
            await_block(block, condition)
            if square and step % 2 == place:
                send_block(block, to_chip(near[1 - place]), condition)
            send_block(block, {"tm": partner}, condition)

    for place, item in enumerate(items):
        if place > 0:
            from_column(item)
            from_near(items[place - 1])
        if place == min(2, len(items) - 1):
            settle()
    from_near(items[-1])
    if square:
        for step, condition, depth, onward in items:
            block = at(depth, corner, core)
            await_block(block, condition)
            send_block(block, {"tm": partner}, condition)
    for of_chip in range(chips):
        for depth in range(blocks):
            await_block(at(depth, of_chip, 1 - core))
    for k in range(1, blocks):
        frm = lax.rem(z + k, blocks)
        pltpu.make_async_copy(source_all.at[frm], source_all.at[frm], source_recv.at[frm]).wait()
    for condition, copy in pending:
        when(condition, copy.wait_send)


def spread(gauge, time, picked, starts, n_time, blocks):
    held = picked.shape[1]
    n = n_time * blocks
    vmem = pl.BlockSpec(memory_space=pltpu.VMEM)
    size = n * (2 * math.prod(gauge.shape) + 4 * math.prod(time.shape))
    landing = vmem if size <= VMEM_ROOM else pl.BlockSpec(memory_space=pl.ANY)
    dma = pltpu.SemaphoreType.DMA
    return pl.pallas_call(
        lambda *refs: spread_kernel(n_time, blocks, held, *refs),
        out_shape=[
            jax.ShapeDtypeStruct((n,) + gauge.shape, gauge.dtype),
            jax.ShapeDtypeStruct((n,) + time.shape, time.dtype),
            jax.ShapeDtypeStruct((blocks,) + picked.shape[1:], picked.dtype),
        ],
        in_specs=[pl.BlockSpec(memory_space=pltpu.SMEM), vmem, vmem, vmem],
        out_specs=[landing] * 3,
        scratch_shapes=[
            pltpu.VMEM(picked.shape, picked.dtype),
            pltpu.VMEM(picked.shape[1:], picked.dtype),
            pltpu.VMEM(picked.shape[1:], picked.dtype),
            dma((2, 4 * n + 8)), dma((2, n)), dma((5,)),
            dma((n_time,)), dma((n_time,)), dma((blocks,)), dma((blocks,)),
        ],
        compiler_params=pltpu.CompilerParams(collective_id=0, has_side_effects=True),
        name="spread",
    )(starts, gauge, time, picked)


def evolve_kernel(planes, rows, blocks, side, start_ref, place_ref, weight_ref, gauge_ref, time_ref,
                  source_ref, out_ref, field, turned, wide):
    which, rounds = pl.program_id(0), pl.program_id(1)
    extent = planes * blocks
    weight = weight_ref[which]
    lane = lax.broadcasted_iota(jnp.int32, (planes, rows, LANES), 2)
    per_row = LANES // side

    def y_up(x):
        turned_lanes = roll(x, -side, 2)
        return jnp.where(lane < LANES - side, turned_lanes, roll(turned_lanes, -1, 1))

    def y_down(x):
        turned_lanes = roll(x, side, 2)
        return jnp.where(lane >= side, turned_lanes, roll(turned_lanes, 1, 1))

    def z_up(x):
        return jnp.where(lane % side == side - 1, roll(x, side - 1, 2), roll(x, -1, 2))

    def z_down(x):
        return jnp.where(lane % side == 0, roll(x, 1 - side, 2), roll(x, 1, 2))

    def gauge(block, direction):
        def link(part, row, column):
            return wide[block, ((part * 3 + direction) * 3 + row) * 3 + column]
        return link

    def shaped(x):
        return x.astype(jnp.float32).reshape(planes, rows, LANES)

    def third_row(u):
        real, imag = [], []
        for c in range(3):
            d, e = (c + 1) % 3, (c + 2) % 3
            real.append(u[0][0][d] * u[0][1][e] - u[1][0][d] * u[1][1][e]
                        - u[0][0][e] * u[0][1][d] + u[1][0][e] * u[1][1][d])
            imag.append(u[0][0][e] * u[1][1][d] + u[1][0][e] * u[0][1][d]
                        - u[0][0][d] * u[1][1][e] - u[1][0][d] * u[0][1][e])
        return real, imag

    def widen(block, nothing):
        for direction in range(3):
            u = [[[shaped(gauge_ref[0, block, ((part * 3 + direction) * 2 + row) * 3 + c])
                   for c in range(3)] for row in range(2)] for part in range(2)]
            for part, extra in enumerate(third_row(u)):
                for row, values in enumerate(u[part] + [extra]):
                    for c in range(3):
                        wide[block, ((part * 3 + direction) * 3 + row) * 3 + c] = values[c]
        return nothing

    def read(ref, first):
        return [[ref[part * 3 + c, pl.ds(first, planes)] for c in range(3)] for part in range(2)]

    def each(fn, vec):
        return [[fn(vec[part][c]) for c in range(3)] for part in range(2)]

    def plus(*vecs):
        return [[sum(v[part][c] for v in vecs[1:]) + vecs[0][part][c] for c in range(3)] for part in range(2)]

    def close(ref):
        for at in range(6):
            ref[at, pl.ds(extent, 1)] = ref[at, pl.ds(0, 1)]

    def hop(src, dst, then):
        last = read(src, extent - planes)
        _, wrapped = apply_both(gauge(blocks - 1, 0), last, last)
        carried = tuple(wrapped[part][c][planes - 1:] for part in range(2) for c in range(3))

        def one_block(block, carry):
            first = block * planes
            here = read(src, first)
            up, down = apply_both(gauge(block, 0), read(src, first + 1), here)
            flat = [down[part][c] for part in range(2) for c in range(3)]
            moved = [jnp.concatenate([low, x[: planes - 1]], axis=0) for low, x in zip(carry, flat)]
            total = plus(up, [moved[:3], moved[3:]])
            up, down = apply_both(gauge(block, 1), each(y_up, here), here)
            total = plus(total, up, each(y_down, down))
            up, down = apply_both(gauge(block, 2), each(z_up, here), here)
            total = plus(total, up, each(z_down, down))
            result = [[here[part][c] + weight * (total[part][c] - 6.0 * here[part][c]) for c in range(3)]
                      for part in range(2)]
            result = then(block, result)
            for part in range(2):
                for c in range(3):
                    dst[part * 3 + c, pl.ds(first, planes)] = result[part][c]
            return tuple(x[planes - 1:] for x in flat)

        lax.fori_loop(0, blocks, one_block, carried)
        close(dst)

    def through_time(block, vec):
        u = [[[shaped(time_ref[0, block, (part * 2 + row) * 3 + c]) for c in range(3)]
              for row in range(2)] for part in range(2)]
        for part, extra in enumerate(third_row(u)):
            u[part].append(extra)
        real, imag = [], []
        for c in range(3):
            real.append(sum(u[0][row][c] * vec[0][row] + u[1][row][c] * vec[1][row] for row in range(3)))
            imag.append(sum(u[0][row][c] * vec[1][row] - u[1][row][c] * vec[0][row] for row in range(3)))
        return [real, imag]

    @pl.when(rounds == 0)
    def _():
        for block in range(blocks):
            for at in range(6):
                value = source_ref[0, block, at].astype(jnp.float32)
                field[at, pl.ds(block * planes, planes)] = value.reshape(planes, rows, LANES)
        close(field)

    lax.fori_loop(0, blocks, widen, 0)
    hop(field, turned, through_time)
    hop(turned, field, lambda block, vec: vec)
    mine = place_ref[0] * planes
    for at in range(6):
        value = field[at, pl.ds(mine, planes)].reshape(planes * rows, LANES)
        out_ref[0, 0, at] = value.astype(jnp.bfloat16)


def evolve(gauge_all, time_all, sources, starts, place, weights, n_time):
    held, blocks = sources.shape[0], sources.shape[1]
    tile = sources.shape[3]
    planes = evolve.planes
    rows = tile // planes
    side = math.isqrt(rows * LANES)

    def at_time(v, r, start, place):
        return (lax.rem(start[v] + r, n_time), 0, 0, 0, 0)

    kernel = lambda *refs: evolve_kernel(planes, rows, blocks, side, *refs)
    extent = planes * blocks
    return pl.pallas_call(
        kernel,
        out_shape=jax.ShapeDtypeStruct((held, n_time, 6, tile, LANES), jnp.bfloat16),
        grid_spec=pltpu.PrefetchScalarGridSpec(
            num_scalar_prefetch=2,
            grid=(held, n_time),
            in_specs=[
                pl.BlockSpec(memory_space=pltpu.SMEM),
                pl.BlockSpec((1,) + gauge_all.shape[1:], at_time),
                pl.BlockSpec((1,) + time_all.shape[1:], at_time),
                pl.BlockSpec((1,) + sources.shape[1:], lambda v, r, start, place: (v, 0, 0, 0, 0)),
            ],
            out_specs=pl.BlockSpec(
                (1, 1, 6, tile, LANES),
                lambda v, r, start, place: (v, lax.rem(start[v] + r, n_time), 0, 0, 0)),
            scratch_shapes=[pltpu.VMEM((6, extent + 1, rows, LANES), jnp.float32)] * 2
            + [pltpu.VMEM((blocks, 54, planes, rows, LANES), jnp.float32)],
        ),
        name="evolve",
    )(starts, place, weights, gauge_all, time_all, sources)


def collect_kernel(blocks, part_ref, out_ref, parts, send_sem, recv_sem, self_sem):
    z = lax.axis_index("space")
    barrier = pltpu.get_barrier_semaphore()
    others = [lax.rem(z + k, blocks) for k in range(1, blocks)]
    for other in others:
        pl.semaphore_signal(barrier, inc=1, device_id={"space": other}, device_id_type=MESH)
    pl.semaphore_wait(barrier, blocks - 1)
    copies = []
    for k, other in enumerate(others):
        copies.append(pltpu.make_async_remote_copy(
            src_ref=part_ref, dst_ref=parts.at[z], send_sem=send_sem.at[k], recv_sem=recv_sem.at[z],
            device_id={"space": other}, device_id_type=MESH))
        copies[-1].start()
    mine = pltpu.make_async_copy(part_ref, parts.at[z], self_sem)
    mine.start()
    mine.wait()
    for other in others:
        pltpu.make_async_copy(parts.at[other], parts.at[other], recv_sem.at[other]).wait()
    for copy in copies:
        copy.wait_send()
    total = parts[0]
    for block in range(1, blocks):
        total = total + parts[block]
    width = out_ref.shape[1]
    kept = total[:, :width]
    for block in range(1, blocks):
        kept = jnp.where(z == block, total[:, block * width:(block + 1) * width], kept)
    out_ref[...] = kept


def collect(partial, blocks):
    rows, columns = partial.shape
    vmem = pl.BlockSpec(memory_space=pltpu.VMEM)
    dma = pltpu.SemaphoreType.DMA
    return pl.pallas_call(
        lambda *refs: collect_kernel(blocks, *refs),
        out_shape=jax.ShapeDtypeStruct((rows, columns // blocks), jnp.float32),
        in_specs=[vmem],
        out_specs=vmem,
        scratch_shapes=[pltpu.VMEM((blocks, rows, columns), jnp.float32),
                        dma((blocks,)), dma((blocks,)), dma],
        compiler_params=pltpu.CompilerParams(collective_id=1, has_side_effects=True),
        name="collect",
    )(partial)


def project(sinks, rounded):
    def dot(a, b):
        return jnp.einsum("ecxs,vcxs->ve", a, b, preferred_element_type=jnp.float32)

    real_part = dot(sinks[0], rounded[:, 0]) + dot(sinks[1], rounded[:, 1])
    imag_part = dot(sinks[0], rounded[:, 1]) - dot(sinks[1], rounded[:, 0])
    return jnp.stack([real_part, imag_part])


def local(gauge_links, time_links, sink_vectors, source_times, source_index, kinetic_coef):
    planes, sites = gauge_links.shape[5:]
    tile = planes * sites // LANES
    n_time = lax.axis_size("tm")
    blocks = lax.axis_size("space")
    my_time = lax.axis_index("tm")
    groups, per_group = kinetic_coef.shape
    count = groups * per_group
    held = -(-count // n_time)
    fill = (0, held * n_time - count)
    start_flat = jnp.pad(jnp.repeat(source_times, per_group), fill)
    index_flat = jnp.pad(source_index.reshape(-1), fill)
    coef_flat = jnp.pad(kinetic_coef.reshape(-1), fill)
    my_sinks = sink_vectors[0]

    mine = lambda x: lax.dynamic_slice_in_dim(x, my_time * held, held)
    starts = mine(start_flat)
    gauge = gauge_links[0, :, :, :2].astype(jnp.bfloat16).reshape(36, tile, LANES)
    time = time_links[0, :, :2].reshape(12, tile, LANES)
    picked = jnp.take(my_sinks, index_flat, axis=1)
    picked = jnp.moveaxis(picked, 1, 0).reshape(n_time, held, 6, tile, LANES)
    gauge_all, time_all, sources = spread(gauge, time, picked, starts, n_time, blocks)
    gauge_all = gauge_all.reshape((n_time, blocks) + gauge.shape)
    time_all = time_all.reshape((n_time, blocks) + time.shape)
    sources = jnp.moveaxis(sources, 0, 1)

    evolve.planes = planes
    place = lax.axis_index("space").astype(jnp.int32)[None]
    evolved = evolve(gauge_all, time_all, sources, starts, place, 0.5 * mine(coef_flat), n_time)
    back = lax.all_to_all(jnp.moveaxis(evolved, 1, 0), "tm", 0, 0, tiled=False)
    rounded = back.reshape(n_time * held, 2, 3, planes, sites)[:count]
    correlations = project(my_sinks, rounded)
    total = collect(correlations.reshape(2 * count, -1), blocks)
    return total.reshape(2, groups, per_group, 1, -1)


def solution(mesh):
    placed = (
        P("tm", None, None, None, None, "space", None),
        P("tm", None, None, None, "space", None),
        P("tm", None, None, None, "space", None),
        P(),
        P(),
        P(),
    )
    return jax.shard_map(
        local,
        mesh=mesh,
        in_specs=placed,
        out_specs=P(None, None, None, "tm", "space"),
        check_vma=False,
    )
```
